32 devices in a mesh: parts: 2 (over y), blk: 4 (over x, core), sub: 4 (over z).
Axes of the slice: x: 2, y: 2, z: 4, core: 2. Of those that a mesh axis runs over, the one named last changes fastest.
Arguments:
- tokens: bfloat16 [256, 4096], P(('parts', 'blk'), 'sub'), parts along dimension 0, may hold values from -6 to 6
- expert_ids: int32 [256, 2], P(('parts', 'blk')), parts along dimension 0, may hold values from 0 to 7, all different within a row; in each aligned block of 32 rows (0 to 31, 32 to 63, ...) at most 16 rows name the same one
- gate_level: int32 [256, 2], P(('parts', 'blk')), parts along dimension 0, may hold values from 0 to 15
- gate_weight: bfloat16 [8, 4096, 8192], P('blk', None, 'sub'), may hold values from -0.09375 to 0.09375
- up_weight: bfloat16 [8, 4096, 8192], P('blk', None, 'sub'), may hold values from -0.09375 to 0.09375
- down_weight: bfloat16 [8, 8192, 4096], P('blk', 'sub'), may hold values from -0.0625 to 0.0625
Outputs:
- mixed_out: bfloat16 [256, 4096], P(('parts', 'blk'), 'sub'), parts along dimension 0
The draws below stay inside these ranges and needn't reach their ends.
There are 2 independent parts, one for each index of `parts`. The reference program is written for one: setup_inputs(seed, part) draws one part's arguments, and reference() takes and returns one part's arrays. A program takes and returns all parts, laid end to end along the dimension named above; an argument that names none is the same for every part. Nothing has to cross between parts.
Inputs may be any that keep to these rules, and one draw needn't show every extreme that they name: `expert_ids`: A token's 2 experts differ. Among the 32 tokens of one index of blk (aligned blocks of tokens), no expert is picked by more than 16 tokens, and in some block some expert is picked by exactly 16.
All inputs are finite; a program needn't handle non-finite values.
Results may differ from the reference program's by a relative error of at most 0.015.
Values may be sent and summed in bfloat16 or wider, within the bound.
A program may use at most 192 MiB of HBM per device.

```python
import math
import jax
import jax.numpy as jnp
import numpy as np
from jax import lax

D = 4096
E = 8
TOP = 2
FF = 8192
LEVELS = 16
TOK_BLK = 32
FSPLIT = 1
SLOTS = 8
SLOT_FF = 8192
CAP = 16
TOKENS = 128
N_BLK = 4


def with_ends(array, rng, smallest, high):
    longest = array.shape.index(max(array.shape))
    spots = []
    for shift in (0, 1):
        where = [jax.random.randint(jax.random.fold_in(rng, axis), (), 0, length) for axis, length in enumerate(array.shape)]
        where[longest] = (where[longest] + shift) % array.shape[longest]
        spots.append(tuple(where))
    return array.at[spots[0]].set(smallest).at[spots[1]].set(high)


def steps_of(stream_key, shape, split, smallest, high):
    def one(dim, parts):
        draws = jax.random.uniform(jax.random.fold_in(jax.random.fold_in(stream_key, 6), dim), (parts,), jnp.float32, smallest / len(split), high / len(split))
        return jnp.repeat(jnp.exp(draws), shape[dim] // parts).reshape((-1,) + (1,) * (len(shape) - dim - 1))

    level = one(*split[0])
    for cut in split[1:]:
        level = level * one(*cut)
    return level


def routed_block(key, own, number, rows, amount, top, bound, slope):
    order = jax.random.permutation(key, amount)
    crowded, ordinary = load_shares(amount, rows * top, bound, slope, True), load_shares(amount, rows * top, bound, slope, False)
    places = jnp.arange(amount)

    def named(sizes, rotation):
        used = int((sizes > 0).sum())
        fixed = max(1, used // 4)
        passed = fixed + (places - fixed + rotation * (used - fixed)) % max(1, amount - fixed)
        return jnp.zeros((amount,), jnp.int32).at[order[jnp.where(places < fixed, places, passed)]].set(jnp.asarray(sizes, jnp.int32))

    sizes = jnp.where(number % 4 == 0, named(crowded, number // 4), named(ordinary, number - number // 4 - 1))
    mixed = jax.random.permutation(jax.random.fold_in(own, 3), amount)
    source_of, sink = mixed[0:amount // 2 * 2:2], mixed[1:amount // 2 * 2:2]
    room = jnp.minimum(sizes[source_of] - 1, bound - sizes[sink]) // 2
    room = jnp.where((source_of == order[0]) | (sink == order[0]) | (sizes[sink] == 0), 0, jnp.maximum(room, 0))
    passed = jax.random.randint(jax.random.fold_in(own, 4), (amount // 2,), 0, 1 << 20) % (room + 1)
    sizes = sizes.at[source_of].add(-passed).at[sink].add(passed)
    labels = jnp.searchsorted(jnp.cumsum(sizes), jnp.arange(rows * top), side="right").astype(jnp.int32)
    listing = labels.reshape(top, rows).T
    listing = listing[jax.random.permutation(jax.random.fold_in(own, 1), rows)]
    rotation = jax.random.randint(jax.random.fold_in(own, 2), (rows, 1), 0, top)
    return jnp.take_along_axis(listing, (jnp.arange(top)[None, :] + rotation) % top, axis=1)


def load_shares(count, total, bound, slope, full):
    weights = [(1 << 20) // math.isqrt(rank ** slope) + 1 for rank in range(1, count + 1)]
    largest = bound if full else min(bound, max(-(-total // count), total * weights[0] // sum(weights)))
    least = 1 if total - largest >= count - 1 else 0
    holding, surplus = [largest] + [least] * (count - 1), total - largest - least * (count - 1)
    while surplus > 0:
        free = [i for i in range(1, count) if holding[i] < largest] or [i for i in range(1, count) if holding[i] < bound]
        pool, budget = sum([weights[i] for i in free]), surplus
        for i in free:
            extra = min(bound - holding[i], max(1, budget * weights[i] // pool), surplus)
            holding[i] = holding[i] + extra
            surplus = surplus - extra
    return np.array(holding)


def centred(key, extent, spread, most, shards=(), kind=jnp.bfloat16):
    entries = jax.random.normal(key, extent, jnp.float32) * spread
    if len(shards) > 0:
        entries = steps_of(key, extent, shards, -0.22, 0.18) * entries
    return jnp.clip(entries, min=-most, max=most).astype(kind)


def setup_inputs(seed: int = 0, part: int = 0) -> dict:
    streams_of = jax.random.split(jax.random.key(seed), 7)
    part_splits = jax.random.split(jax.random.fold_in(streams_of[6], part), 7)
    tokens = centred(part_splits[0], (TOKENS, D), 1.0, 6.0, ((0, 4), (1, 4)))
    expert_ids_keys = jax.random.split(jax.random.fold_in(part_splits[1], 1), TOKENS // TOK_BLK)
    expert_ids_turns = jax.random.permutation(jax.random.fold_in(part_splits[1], 3), TOKENS // TOK_BLK)
    expert_ids = jax.vmap(lambda own, number: routed_block(jax.random.fold_in(part_splits[1], 2), own, number, TOK_BLK, E, TOP, CAP, 2))(expert_ids_keys, expert_ids_turns).reshape((TOKENS, TOP))
    gate_level = with_ends(jax.random.randint(part_splits[2], (TOKENS, TOP), 0, LEVELS), jax.random.fold_in(part_splits[2], 1), 0, LEVELS - 1).astype(jnp.int32)
    gate_weight = centred(streams_of[3], (SLOTS, D, SLOT_FF), D ** -0.5, 0.09375, ((0, 4), (2, 4)))
    up_weight = centred(streams_of[4], (SLOTS, D, SLOT_FF), D ** -0.5, 0.09375, ((0, 4), (2, 4)))
    down_weight = centred(streams_of[5], (SLOTS, SLOT_FF, D), FF ** -0.5, 0.0625, ((0, 4), (1, 4)))
    return {"tokens": tokens, "expert_ids": expert_ids, "gate_level": gate_level, "gate_weight": gate_weight, "up_weight": up_weight, "down_weight": down_weight}


def reference(tokens, expert_ids, gate_level, gate_weight, up_weight, down_weight):
    picked = expert_ids.reshape(N_BLK, TOK_BLK * TOP)
    onehot = (picked[:, :, None] == jnp.arange(E, dtype=jnp.int32)[None, None, :]).astype(jnp.int32)
    ranking = jnp.sum((jnp.cumsum(onehot, axis=1) - onehot) * onehot, axis=2)
    block_index = jnp.arange(N_BLK, dtype=jnp.int32)[:, None]
    position = (block_index * CAP + ranking).reshape(-1).astype(jnp.int32)
    flat_expert = expert_ids.reshape(-1).astype(jnp.int32)
    token_index = jnp.repeat(jnp.arange(TOKENS, dtype=jnp.int32), TOP)
    row_table = jnp.full((E, N_BLK * CAP), TOKENS, jnp.int32).at[flat_expert, position].set(token_index)
    padded = jnp.concatenate([tokens, jnp.zeros((1, D), tokens.dtype)], axis=0)

    def one_slot(slot_index):
        expert = slot_index % E
        slot_rows = padded[row_table[expert]]
        gate_acts = jnp.dot(slot_rows, gate_weight[slot_index], preferred_element_type=jnp.float32)
        up_acts = jnp.dot(slot_rows, up_weight[slot_index], preferred_element_type=jnp.float32)
        hidden = (jax.nn.silu(gate_acts) * up_acts).astype(jnp.bfloat16)
        return jnp.dot(hidden, down_weight[slot_index], preferred_element_type=jnp.float32).astype(jnp.bfloat16)

    slot_out = lax.map(one_slot, jnp.arange(SLOTS, dtype=jnp.int32))
    expert_sum = jnp.sum(slot_out.astype(jnp.float32).reshape(FSPLIT, E, N_BLK * CAP, D), axis=0)
    levels = gate_level.astype(jnp.float32) + 1.0
    shares = levels / jnp.sum(levels, axis=1, keepdims=True)
    gathered = expert_sum[flat_expert, position].reshape(TOKENS, TOP, D)
    mixed_out = jnp.sum(gathered * shares[:, :, None], axis=1)
    return mixed_out.astype(jnp.bfloat16)
```

```python
import functools

import jax
import jax.numpy as jnp
from jax import lax
from jax.sharding import PartitionSpec as P

from jax.experimental import pallas as pl
from jax.experimental.pallas import tpu as pltpu

E = 8
TOP = 2
CAP = 16
BF16 = jnp.bfloat16
F32 = jnp.float32
TILE = 512
AHEAD = 6


def shards(tokens, expert_ids, gate_level, gate_weight, up_weight, down_weight):
    block_count = lax.axis_size("blk")
    sub_count = lax.axis_size("sub")
    local_slots = gate_weight.shape[0]
    hidden_width = gate_weight.shape[2]
    slot_count = local_slots * block_count
    halves = slot_count // E
    token_rows = tokens.shape[0]
    feature_width = tokens.shape[1]
    buffer_width = slot_count * CAP
    received_rows = block_count * CAP
    picked = expert_ids.reshape(-1)
    onehot = (picked[:, None] == jnp.arange(E, dtype=jnp.int32)[None, :]).astype(jnp.int32)
    ranking = jnp.sum((jnp.cumsum(onehot, axis=0) - onehot) * onehot, axis=1)
    columns = (
        picked[:, None] * CAP
        + (jnp.arange(halves, dtype=jnp.int32) * E)[None, :] * CAP
        + ranking[:, None]
    )
    columns = columns.reshape(token_rows, TOP * halves)
    matches = columns[:, :, None] == jnp.arange(buffer_width, dtype=jnp.int32)[None, None, :]
    levels = gate_level.astype(jnp.float32) + 1.0
    shares = levels / jnp.sum(levels, axis=1, keepdims=True)
    shares_wide = jnp.repeat(shares, halves, axis=1)
    combine_weights = jnp.sum(matches.astype(jnp.float32) * shares_wide[:, :, None], axis=1)
    chosen = jnp.any(matches, axis=1).astype(jnp.bfloat16)
    outgoing = lax.dot_general(
        chosen, tokens, (((0,), (0,)), ((), ())), preferred_element_type=jnp.float32
    )
    outgoing = outgoing.astype(jnp.bfloat16).reshape(slot_count, CAP, feature_width)
    copies = jnp.broadcast_to(
        outgoing.reshape(block_count, 1, local_slots, CAP, feature_width),
        (block_count, sub_count, local_slots, CAP, feature_width),
    )
    copies = copies.reshape(block_count * sub_count, local_slots, CAP, feature_width)
    arrived = lax.all_to_all(copies, ("blk", "sub"), split_axis=0, concat_axis=0, tiled=True)
    arrived = arrived.reshape(block_count, sub_count, local_slots, CAP, feature_width)
    gate_split = gate_weight.reshape(local_slots, sub_count, feature_width, hidden_width)
    up_split = up_weight.reshape(local_slots, sub_count, feature_width, hidden_width)
    gate_acts = jnp.einsum(
        "bsncd,nsdf->nbcf", arrived, gate_split, preferred_element_type=jnp.float32
    )
    up_acts = jnp.einsum("bsncd,nsdf->nbcf", arrived, up_split, preferred_element_type=jnp.float32)
    gate_acts = gate_acts.reshape(local_slots, received_rows, hidden_width)
    up_acts = up_acts.reshape(local_slots, received_rows, hidden_width)
    hidden = (jax.nn.silu(gate_acts) * up_acts).astype(jnp.bfloat16)
    full_out = jnp.einsum("nrf,nfd->nrd", hidden, down_weight, preferred_element_type=jnp.float32)
    local_out = lax.psum_scatter(
        full_out.astype(jnp.bfloat16), "sub", scatter_dimension=2, tiled=True
    )
    home_rows = lax.all_to_all(local_out, "blk", split_axis=1, concat_axis=0, tiled=True)
    home_flat = home_rows.reshape(buffer_width, feature_width).astype(jnp.float32)
    mixed_out = jnp.dot(
        combine_weights,
        home_flat,
        precision=lax.Precision.HIGHEST,
        preferred_element_type=jnp.float32,
    )
    return mixed_out.astype(jnp.bfloat16)


def flip(index, mask, count):
    total, bit = 0, 1
    while bit < count:
        digit = (index // bit) % 2
        total = total + bit * ((1 - digit) if mask & bit else digit)
        bit *= 2
    return total


def fused(
    parts, blks, subs, tokens, ids, levels, gate_hbm, up_hbm, down_hbm, out,
    taken, picked, rows, gate, up, down, gate_sum, up_sum, hidden, made, home, mixed, landed,
    load_sem, tok_send, tok_recv, pick_send, pick_recv, made_send, made_recv, mix_send, mix_recv,
):
    plane = parts * blks
    part, blk, sub = lax.axis_index("parts"), lax.axis_index("blk"), lax.axis_index("sub")
    mine = blk * parts + part
    width = tokens.shape[1]
    block_rows = tokens.shape[0]
    units = hidden.shape[1]

    def at(slot, depth):
        return {"parts": slot % parts, "blk": slot // parts, "sub": depth}

    quarters = [flip(sub, j, subs) for j in range(subs)]
    peers = [flip(mine, k, plane) for k in range(plane)]

    loads = []
    for j in range(subs):
        span = pl.ds(pl.multiple_of(quarters[j] * width, width), width)
        loads.append(pltpu.make_async_copy(gate_hbm.at[part, span, :], gate.at[j], load_sem.at[2 * j]))
        loads.append(pltpu.make_async_copy(up_hbm.at[part, span, :], up.at[j], load_sem.at[2 * j + 1]))
    for i, j in enumerate(reversed(range(subs))):
        span = pl.ds(pl.multiple_of(quarters[j] * width, width), width)
        loads.append(pltpu.make_async_copy(down_hbm.at[part, :, span], down.at[j], load_sem.at[2 * subs + i]))
    for load in loads[:AHEAD]:
        load.start()

    barrier = pltpu.get_barrier_semaphore()
    for k in range(1, plane):
        pl.semaphore_signal(barrier, inc=1, device_id=at(peers[k], sub), device_id_type=pl.DeviceIdType.MESH)
    for j in range(1, subs):
        pl.semaphore_signal(barrier, inc=1, device_id=at(mine, quarters[j]), device_id_type=pl.DeviceIdType.MESH)

    columns = E * CAP
    column = lax.broadcasted_iota(jnp.int32, (block_rows, columns), 1)
    expert, place = column // CAP, column % CAP
    first = jnp.broadcast_to(ids[:, 0:1], (block_rows, columns)) == expert
    second = jnp.broadcast_to(ids[:, 1:2], (block_rows, columns)) == expert
    named = jnp.where(first | second, 1.0, 0.0).astype(F32)
    before = lax.broadcasted_iota(jnp.int32, (block_rows, block_rows), 0) > lax.broadcasted_iota(
        jnp.int32, (block_rows, block_rows), 1
    )
    rank = jnp.dot(jnp.where(before, 1.0, 0.0).astype(BF16), named.astype(BF16), preferred_element_type=F32)
    here = jnp.where(rank == place.astype(F32), named, 0.0)
    chosen = here.astype(BF16)
    level = levels[...].astype(F32) + 1.0
    share = level / (level[:, 0:1] + level[:, 1:2])
    weight = here * jnp.where(
        first,
        jnp.broadcast_to(share[:, 0:1], (block_rows, columns)),
        jnp.broadcast_to(share[:, 1:2], (block_rows, columns)),
    )
    weight_high = weight.astype(BF16)
    weight_low = (weight - weight_high.astype(F32)).astype(BF16)

    pl.semaphore_wait(barrier, plane + subs - 2)

    tok_copies = {}
    for j in range(1, subs):
        tok_copies[j] = pltpu.make_async_remote_copy(
            src_ref=tokens, dst_ref=taken.at[j], send_sem=tok_send.at[j], recv_sem=tok_recv.at[j],
            device_id=at(mine, quarters[j]), device_id_type=pl.DeviceIdType.MESH,
        )
        tok_copies[j].start()

    def dispatch(j):
        if j > 0:
            tok_copies[j].wait_recv()
        block = tokens[...] if j == 0 else taken[j]
        sent = lax.dot_general(chosen, block, (((0,), (0,)), ((), ())), preferred_element_type=F32)
        picked[j] = sent.astype(BF16).reshape(plane, CAP, width)
        copies = []
        for k in reversed(range(1, plane)):
            copy = pltpu.make_async_remote_copy(
                src_ref=picked.at[j, peers[k]], dst_ref=rows.at[j, mine],
                send_sem=pick_send.at[j, k], recv_sem=pick_recv.at[j, k],
                device_id=at(peers[k], sub), device_id_type=pl.DeviceIdType.MESH,
            )
            copy.start()
            copies.append(copy)
        rows[j, mine] = picked[j, mine]
        return copies

    pick_copies = [dispatch(j) for j in range(subs)]

    started = AHEAD
    for j in range(subs):
        for copy in pick_copies[j]:
            copy.wait_recv()
        for i in (2 * j, 2 * j + 1):
            loads[i].wait()
            if started < len(loads):
                loads[started].start()
                started += 1

        @pl.loop(0, units // TILE)
        def _(step, j=j):
            span = pl.ds(pl.multiple_of(step * TILE, TILE), TILE)
            x = rows[j].reshape(plane * CAP, width)
            g = jnp.dot(x, gate[j, :, span], preferred_element_type=F32)
            u = jnp.dot(x, up[j, :, span], preferred_element_type=F32)
            if j > 0:
                g = g + gate_sum[:, span]
                u = u + up_sum[:, span]
            if j < subs - 1:
                gate_sum[:, span] = g
                up_sum[:, span] = u
            else:
                hidden[:, span] = (g / (1.0 + jnp.exp(-g)) * u).astype(BF16)

    made_copies = {}
    mix_copies = {}

    def ship(j):
        copies = []
        for k in reversed(range(1, plane)):
            copy = pltpu.make_async_remote_copy(
                src_ref=made.at[j, peers[k]], dst_ref=home.at[j, mine],
                send_sem=made_send.at[j, k], recv_sem=made_recv.at[j, k],
                device_id=at(peers[k], sub), device_id_type=pl.DeviceIdType.MESH,
            )
            copy.start()
            copies.append(copy)
        home[j, mine] = made[j, mine]
        made_copies[j] = copies

    def combine(j):
        for copy in made_copies[j]:
            copy.wait_recv()
        block = home[j].reshape(plane * CAP, width)
        return jnp.dot(weight_high, block, preferred_element_type=F32) + jnp.dot(
            weight_low, block, preferred_element_type=F32
        )

    for i, j in enumerate(reversed(range(subs))):
        loads[2 * subs + i].wait()
        if started < len(loads):
            loads[started].start()
            started += 1

        @pl.loop(0, width // TILE)
        def _(step, j=j):
            span = pl.ds(pl.multiple_of(step * TILE, TILE), TILE)
            y = jnp.dot(hidden[...], down[j, :, span], preferred_element_type=F32)
            made[j, :, :, span] = y.astype(BF16).reshape(plane, CAP, TILE)

        ship(j)

    for j in reversed(range(1, subs)):
        mixed[j] = combine(j).astype(BF16)
        mix_copies[j] = pltpu.make_async_remote_copy(
            src_ref=mixed.at[j], dst_ref=landed.at[j], send_sem=mix_send.at[j], recv_sem=mix_recv.at[j],
            device_id=at(mine, quarters[j]), device_id_type=pl.DeviceIdType.MESH,
        )
        mix_copies[j].start()
    total = combine(0)
    for j in reversed(range(1, subs)):
        mix_copies[j].wait_recv()
        total = total + landed[j].astype(F32)
    out[...] = total.astype(BF16)

    for j in range(1, subs):
        tok_copies[j].wait_send()
        mix_copies[j].wait_send()
    for j in range(subs):
        for copy in pick_copies[j] + made_copies[j]:
            copy.wait_send()


def shared_shards(parts, blks, subs, tokens, expert_ids, gate_level, gate_weight, up_weight, down_weight):
    block_rows, width = tokens.shape
    plane = parts * blks
    units = gate_weight.shape[2]
    vmem = pl.BlockSpec(memory_space=pltpu.VMEM)
    hbm = pl.BlockSpec(memory_space=pl.ANY)
    dma = pltpu.SemaphoreType.DMA
    return pl.pallas_call(
        functools.partial(fused, parts, blks, subs),
        out_shape=jax.ShapeDtypeStruct((block_rows, width), BF16),
        in_specs=[vmem, vmem, vmem, hbm, hbm, hbm],
        out_specs=vmem,
        scratch_shapes=[
            pltpu.VMEM((subs, block_rows, width), BF16),
            pltpu.VMEM((subs, plane, CAP, width), BF16),
            pltpu.VMEM((subs, plane, CAP, width), BF16),
            pltpu.VMEM((subs, width, units), BF16),
            pltpu.VMEM((subs, width, units), BF16),
            pltpu.VMEM((subs, units, width), BF16),
            pltpu.VMEM((plane * CAP, units), F32),
            pltpu.VMEM((plane * CAP, units), F32),
            pltpu.VMEM((plane * CAP, units), BF16),
            pltpu.VMEM((subs, plane, CAP, width), BF16),
            pltpu.VMEM((subs, plane, CAP, width), BF16),
            pltpu.VMEM((subs, block_rows, width), BF16),
            pltpu.VMEM((subs, block_rows, width), BF16),
            dma((3 * subs,)),
            dma((subs,)), dma((subs,)),
            dma((subs, plane)), dma((subs, plane)),
            dma((subs, plane)), dma((subs, plane)),
            dma((subs,)), dma((subs,)),
        ],
        compiler_params=pltpu.CompilerParams(
            collective_id=0, has_side_effects=True, vmem_limit_bytes=67043328
        ),
    )(tokens, expert_ids, gate_level, gate_weight, up_weight, down_weight)


def routed(parts, blks, subs, tokens, expert_ids, gate_level, gate_weight, up_weight, down_weight):
    plane = parts * blks
    width = tokens.shape[1]
    units = gate_weight.shape[2]
    fits = gate_weight.shape[0] == parts and plane == E and plane & (plane - 1) == 0
    fits = fits and subs & (subs - 1) == 0 and width % TILE == 0 and units % TILE == 0
    fits = fits and tokens.shape[0] == 2 * CAP
    arrays = (tokens, expert_ids, gate_level, gate_weight, up_weight, down_weight)
    return shared_shards(parts, blks, subs, *arrays) if fits else shards(*arrays)


def solution(mesh):
    sizes = (mesh.shape["parts"], mesh.shape["blk"], mesh.shape["sub"])
    return jax.shard_map(
        functools.partial(routed, *sizes),
        mesh=mesh,
        in_specs=(
            P(("parts", "blk"), "sub"),
            P(("parts", "blk"), None),
            P(("parts", "blk"), None),
            P("blk", None, "sub"),
            P("blk", None, "sub"),
            P("blk", "sub", None),
        ),
        out_specs=P(("parts", "blk"), "sub"),
        check_vma=False,
    )
```

```python
import functools

import jax
import jax.numpy as jnp
from jax import lax
from jax.sharding import PartitionSpec as P

from jax.experimental import pallas as pl
from jax.experimental.pallas import tpu as pltpu

E = 8
TOP = 2
CAP = 16
BF16 = jnp.bfloat16
F32 = jnp.float32
TILE = 1024
AHEAD = 6


def shards(tokens, expert_ids, gate_level, gate_weight, up_weight, down_weight):
    block_count = lax.axis_size("blk")
    sub_count = lax.axis_size("sub")
    local_slots = gate_weight.shape[0]
    hidden_width = gate_weight.shape[2]
    slot_count = local_slots * block_count
    halves = slot_count // E
    token_rows = tokens.shape[0]
    feature_width = tokens.shape[1]
    buffer_width = slot_count * CAP
    received_rows = block_count * CAP
    picked = expert_ids.reshape(-1)
    onehot = (picked[:, None] == jnp.arange(E, dtype=jnp.int32)[None, :]).astype(jnp.int32)
    ranking = jnp.sum((jnp.cumsum(onehot, axis=0) - onehot) * onehot, axis=1)
    columns = (
        picked[:, None] * CAP
        + (jnp.arange(halves, dtype=jnp.int32) * E)[None, :] * CAP
        + ranking[:, None]
    )
    columns = columns.reshape(token_rows, TOP * halves)
    matches = columns[:, :, None] == jnp.arange(buffer_width, dtype=jnp.int32)[None, None, :]
    levels = gate_level.astype(jnp.float32) + 1.0
    shares = levels / jnp.sum(levels, axis=1, keepdims=True)
    shares_wide = jnp.repeat(shares, halves, axis=1)
    combine_weights = jnp.sum(matches.astype(jnp.float32) * shares_wide[:, :, None], axis=1)
    chosen = jnp.any(matches, axis=1).astype(jnp.bfloat16)
    outgoing = lax.dot_general(
        chosen, tokens, (((0,), (0,)), ((), ())), preferred_element_type=jnp.float32
    )
    outgoing = outgoing.astype(jnp.bfloat16).reshape(slot_count, CAP, feature_width)
    copies = jnp.broadcast_to(
        outgoing.reshape(block_count, 1, local_slots, CAP, feature_width),
        (block_count, sub_count, local_slots, CAP, feature_width),
    )
    copies = copies.reshape(block_count * sub_count, local_slots, CAP, feature_width)
    arrived = lax.all_to_all(copies, ("blk", "sub"), split_axis=0, concat_axis=0, tiled=True)
    arrived = arrived.reshape(block_count, sub_count, local_slots, CAP, feature_width)
    gate_split = gate_weight.reshape(local_slots, sub_count, feature_width, hidden_width)
    up_split = up_weight.reshape(local_slots, sub_count, feature_width, hidden_width)
    gate_acts = jnp.einsum(
        "bsncd,nsdf->nbcf", arrived, gate_split, preferred_element_type=jnp.float32
    )
    up_acts = jnp.einsum("bsncd,nsdf->nbcf", arrived, up_split, preferred_element_type=jnp.float32)
    gate_acts = gate_acts.reshape(local_slots, received_rows, hidden_width)
    up_acts = up_acts.reshape(local_slots, received_rows, hidden_width)
    hidden = (jax.nn.silu(gate_acts) * up_acts).astype(jnp.bfloat16)
    full_out = jnp.einsum("nrf,nfd->nrd", hidden, down_weight, preferred_element_type=jnp.float32)
    local_out = lax.psum_scatter(
        full_out.astype(jnp.bfloat16), "sub", scatter_dimension=2, tiled=True
    )
    home_rows = lax.all_to_all(local_out, "blk", split_axis=1, concat_axis=0, tiled=True)
    home_flat = home_rows.reshape(buffer_width, feature_width).astype(jnp.float32)
    mixed_out = jnp.dot(
        combine_weights,
        home_flat,
        precision=lax.Precision.HIGHEST,
        preferred_element_type=jnp.float32,
    )
    return mixed_out.astype(jnp.bfloat16)


def flip(index, mask, count):
    total, bit = 0, 1
    while bit < count:
        digit = (index // bit) % 2
        total = total + bit * ((1 - digit) if mask & bit else digit)
        bit *= 2
    return total


def fused(
    parts, blks, subs, tokens_hbm, ids, levels, gate_hbm, up_hbm, down_hbm, out,
    taken, picked, rows, gate, up, down, gate_sum, up_sum, hidden, made, home, mixed, landed,
    load_sem, own_sem, tok_send, tok_recv, pick_send, pick_recv, made_send, made_recv, mix_send, mix_recv, relay_send, relay_recv,
):
    plane = parts * blks
    part, blk, sub = lax.axis_index("parts"), lax.axis_index("blk"), lax.axis_index("sub")
    mine = blk * parts + part
    block_rows, width = tokens_hbm.shape
    units = hidden.shape[1]

    def at(slot, depth):
        return {"parts": slot % parts, "blk": slot // parts, "sub": depth}

    near = width // 4
    far = pl.ds(near, width - near)
    quarters = [flip(sub, j, subs) for j in range(subs)]
    peers = [flip(mine, k, plane) for k in range(plane)]

    own = pltpu.make_async_copy(tokens_hbm, taken.at[0], own_sem)
    own.start()
    barrier = pltpu.get_barrier_semaphore()
    for k in range(1, plane):
        pl.semaphore_signal(barrier, inc=1, device_id=at(peers[k], sub), device_id_type=pl.DeviceIdType.MESH)
    for j in range(1, subs):
        pl.semaphore_signal(barrier, inc=1, device_id=at(mine, quarters[j]), device_id_type=pl.DeviceIdType.MESH)

    loads = []
    for j in range(subs):
        span = pl.ds(pl.multiple_of(quarters[j] * width, width), width)
        loads.append(pltpu.make_async_copy(gate_hbm.at[part, span, :], gate.at[j], load_sem.at[2 * j]))
        loads.append(pltpu.make_async_copy(up_hbm.at[part, span, :], up.at[j], load_sem.at[2 * j + 1]))
    for i, j in enumerate(reversed(range(subs))):
        span = pl.ds(pl.multiple_of(quarters[j] * width, width), width)
        loads.append(pltpu.make_async_copy(down_hbm.at[part, :, span], down.at[j], load_sem.at[2 * subs + i]))
    for load in loads[:AHEAD]:
        load.start()

    lines = E * CAP
    line = lax.broadcasted_iota(jnp.int32, (lines, block_rows), 0)
    expert, place = line // CAP, line % CAP
    first = jnp.broadcast_to(ids[0:1, :], (lines, block_rows)) == expert
    second = jnp.broadcast_to(ids[1:2, :], (lines, block_rows)) == expert
    named = jnp.where(first | second, 1.0, 0.0).astype(F32)
    before = lax.broadcasted_iota(jnp.int32, (block_rows, block_rows), 0) < lax.broadcasted_iota(
        jnp.int32, (block_rows, block_rows), 1
    )
    rank = jnp.dot(named.astype(BF16), jnp.where(before, 1.0, 0.0).astype(BF16), preferred_element_type=F32)
    here = jnp.where(rank == place.astype(F32), named, 0.0)
    chosen = here.astype(BF16)

    own.wait()
    pl.semaphore_wait(barrier, plane + subs - 2)

    tok_copies = {}
    for j in range(1, subs):
        tok_copies[j] = pltpu.make_async_remote_copy(
            src_ref=taken.at[0, :, far], dst_ref=taken.at[j, :, far], send_sem=tok_send.at[j], recv_sem=tok_recv.at[j],
            device_id=at(mine, quarters[j]), device_id_type=pl.DeviceIdType.MESH,
        )
        tok_copies[j].start()

    half = width // 2
    spans_in = [(0, 0, near), (0, near, width - near)]
    spans_in += [(j, near, width - near) for j in range(1, subs - 1)]
    spans_in += [(subs - 1, near, half - near), (subs - 1, half, half)]
    spans_out = [(subs - 1, 0, half), (subs - 1, half, half)] + [(j, 0, width) for j in reversed(range(subs - 1))]

    def dispatch(n, j, start, size):
        span = pl.ds(start, size)
        if j > 0 and start == near:
            tok_copies[j].wait_recv()
        sent = jnp.dot(chosen, taken[j, :, span], preferred_element_type=F32)
        picked[j, :, :, span] = sent.astype(BF16).reshape(plane, CAP, size)
        copies = []
        for k in reversed(range(1, plane)):
            copy = pltpu.make_async_remote_copy(
                src_ref=picked.at[j, peers[k], :, span], dst_ref=rows.at[j, mine, :, span],
                send_sem=pick_send.at[n, k], recv_sem=pick_recv.at[n, k],
                device_id=at(peers[k], sub), device_id_type=pl.DeviceIdType.MESH,
            )
            copy.start()
            copies.append(copy)
        rows[j, mine, :, span] = picked[j, mine, :, span]
        return copies

    pick_copies = [dispatch(n, *piece) for n, piece in enumerate(spans_in[:2])]
    for copy in pick_copies[0]:
        copy.wait_recv()
    relays = {}
    for j in range(1, subs):
        relays[j] = pltpu.make_async_remote_copy(
            src_ref=rows.at[0, :, :, pl.ds(0, near)], dst_ref=rows.at[j, :, :, pl.ds(0, near)],
            send_sem=relay_send.at[j], recv_sem=relay_recv.at[j],
            device_id=at(mine, quarters[j]), device_id_type=pl.DeviceIdType.MESH,
        )
        relays[j].start()
    pick_copies += [dispatch(n + 2, *piece) for n, piece in enumerate(spans_in[2:])]

    level = levels[...].astype(F32) + 1.0
    share = level / (level[0:1, :] + level[1:2, :])
    weight = here * jnp.where(
        first,
        jnp.broadcast_to(share[0:1, :], (lines, block_rows)),
        jnp.broadcast_to(share[1:2, :], (lines, block_rows)),
    )
    weight = weight.T
    weight_high = weight.astype(BF16)
    weight_low = (weight - weight_high.astype(F32)).astype(BF16)

    started = AHEAD
    spans_used = [(j, 0, width) for j in range(subs - 1)] + [(subs - 1, 0, half), (subs - 1, half, half)]
    for n, (j, start, size) in enumerate(spans_used):
        if start == 0:
            if j > 0:
                relays[j].wait_recv()
            for i in (2 * j, 2 * j + 1):
                loads[i].wait()
                if started < len(loads):
                    loads[started].start()
                    started += 1
        for copy in pick_copies[n + 1]:
            copy.wait_recv()

        @pl.loop(0, units // TILE)
        def _(step, n=n, j=j, depth=pl.ds(start, size)):
            span = pl.ds(pl.multiple_of(step * TILE, TILE), TILE)
            x = rows[j, :, :, depth].reshape(plane * CAP, depth.size)
            g = jnp.dot(x, gate[j, depth, span], preferred_element_type=F32)
            u = jnp.dot(x, up[j, depth, span], preferred_element_type=F32)
            if n > 0:
                g = g + gate_sum[:, span]
                u = u + up_sum[:, span]
            if n < len(spans_used) - 1:
                gate_sum[:, span] = g
                up_sum[:, span] = u
            else:
                hidden[:, span] = (g / (1.0 + jnp.exp(-g)) * u).astype(BF16)

    made_copies = {}
    mix_copies = {}

    def ship(n, j, span):
        copies = []
        for k in reversed(range(1, plane)):
            copy = pltpu.make_async_remote_copy(
                src_ref=made.at[j, peers[k], :, span], dst_ref=home.at[j, mine, :, span],
                send_sem=made_send.at[n, k], recv_sem=made_recv.at[n, k],
                device_id=at(peers[k], sub), device_id_type=pl.DeviceIdType.MESH,
            )
            copy.start()
            copies.append(copy)
        home[j, mine, :, span] = made[j, mine, :, span]
        made_copies.setdefault(j, []).extend(copies)

    def combine(j):
        for copy in made_copies[j]:
            copy.wait_recv()
        block = home[j].reshape(plane * CAP, width)
        return jnp.dot(weight_high, block, preferred_element_type=F32) + jnp.dot(
            weight_low, block, preferred_element_type=F32
        )

    for n, (j, start, size) in enumerate(spans_out):
        if start == 0:
            loads[2 * subs + subs - 1 - j].wait()
            if started < len(loads):
                loads[started].start()
                started += 1
        step = size // 2

        @pl.loop(0, 2)
        def _(turn, j=j, start=start, step=step):
            span = pl.ds(pl.multiple_of(start + turn * step, step), step)
            y = jnp.dot(hidden[...], down[j, :, span], preferred_element_type=F32)
            made[j, :, :, span] = y.astype(BF16).reshape(plane, CAP, step)

        ship(n, j, pl.ds(start, size))

    for j in reversed(range(1, subs)):
        mixed[j] = combine(j).astype(BF16)
        mix_copies[j] = pltpu.make_async_remote_copy(
            src_ref=mixed.at[j], dst_ref=landed.at[j], send_sem=mix_send.at[j], recv_sem=mix_recv.at[j],
            device_id=at(mine, quarters[j]), device_id_type=pl.DeviceIdType.MESH,
        )
        mix_copies[j].start()
    total = combine(0)
    for j in reversed(range(1, subs)):
        mix_copies[j].wait_recv()
        total = total + landed[j].astype(F32)
    out[...] = total.astype(BF16)

    for j in range(1, subs):
        tok_copies[j].wait_send()
        relays[j].wait_send()
        mix_copies[j].wait_send()
    for copies in pick_copies + list(made_copies.values()):
        for copy in copies:
            copy.wait_send()


def shared_shards(parts, blks, subs, tokens, expert_ids, gate_level, gate_weight, up_weight, down_weight):
    block_rows, width = tokens.shape
    plane = parts * blks
    units = gate_weight.shape[2]
    vmem = pl.BlockSpec(memory_space=pltpu.VMEM)
    hbm = pl.BlockSpec(memory_space=pl.ANY)
    dma = pltpu.SemaphoreType.DMA
    return pl.pallas_call(
        functools.partial(fused, parts, blks, subs),
        out_shape=jax.ShapeDtypeStruct((block_rows, width), BF16),
        in_specs=[hbm, vmem, vmem, hbm, hbm, hbm],
        out_specs=vmem,
        scratch_shapes=[
            pltpu.VMEM((subs, block_rows, width), BF16),
            pltpu.VMEM((subs, plane, CAP, width), BF16),
            pltpu.VMEM((subs, plane, CAP, width), BF16),
            pltpu.VMEM((subs, width, units), BF16),
            pltpu.VMEM((subs, width, units), BF16),
            pltpu.VMEM((subs, units, width), BF16),
            pltpu.VMEM((plane * CAP, units), F32),
            pltpu.VMEM((plane * CAP, units), F32),
            pltpu.VMEM((plane * CAP, units), BF16),
            pltpu.VMEM((subs, plane, CAP, width), BF16),
            pltpu.VMEM((subs, plane, CAP, width), BF16),
            pltpu.VMEM((subs, block_rows, width), BF16),
            pltpu.VMEM((subs, block_rows, width), BF16),
            dma((3 * subs,)), pltpu.SemaphoreType.DMA,
            dma((subs,)), dma((subs,)),
            dma((subs + 2, plane)), dma((subs + 2, plane)),
            dma((subs + 1, plane)), dma((subs + 1, plane)),
            dma((subs,)), dma((subs,)),
            dma((subs,)), dma((subs,)),
        ],
        compiler_params=pltpu.CompilerParams(
            collective_id=0, has_side_effects=True, vmem_limit_bytes=67043328
        ),
    )(tokens, expert_ids.T, gate_level.T, gate_weight, up_weight, down_weight)


def routed(parts, blks, subs, tokens, expert_ids, gate_level, gate_weight, up_weight, down_weight):
    plane = parts * blks
    width = tokens.shape[1]
    units = gate_weight.shape[2]
    fits = gate_weight.shape[0] == parts and plane == E and plane & (plane - 1) == 0
    fits = fits and subs & (subs - 1) == 0 and width % TILE == 0 and units % TILE == 0
    fits = fits and tokens.shape[0] == 2 * CAP
    arrays = (tokens, expert_ids, gate_level, gate_weight, up_weight, down_weight)
    return shared_shards(parts, blks, subs, *arrays) if fits else shards(*arrays)


def solution(mesh):
    sizes = (mesh.shape["parts"], mesh.shape["blk"], mesh.shape["sub"])
    return jax.shard_map(
        functools.partial(routed, *sizes),
        mesh=mesh,
        in_specs=(
            P(("parts", "blk"), "sub"),
            P(("parts", "blk"), None),
            P(("parts", "blk"), None),
            P("blk", None, "sub"),
            P("blk", None, "sub"),
            P("blk", "sub", None),
        ),
        out_specs=P(("parts", "blk"), "sub"),
        check_vma=False,
    )
```
